32 devices in a mesh: b: 4 (over z), a: 8 (over y, x, core).
Axes of the slice: x: 2, y: 2, z: 4, core: 2. Of those that a mesh axis runs over, the one named last changes fastest.
Arguments:
- u: float32 [256, 256, 256], P(None, 'a', 'b')
- g: float32 [136, 256, 256], P('a', 'b')
Outputs:
- output: float32 [256, 256, 256], P(None, 'a', 'b')
All inputs are finite; a program needn't handle non-finite values.
Results may differ from the reference program's by a relative error of at most 0.001.
Values are sent between devices in bfloat16 or wider.
A program may use at most 1 GiB of HBM per device.

```python
import math
import jax
import jax.numpy as jnp
from jax import lax

N = 256
KX = 136

HI = lax.Precision.HIGHEST


def _trig(rows, cols):
    r = jnp.arange(rows, dtype=jnp.int32)[:, None]
    c = jnp.arange(cols, dtype=jnp.int32)[None, :]
    ang = ((r * c) % N).astype(jnp.float32) * (2.0 * math.pi / N)
    return jnp.cos(ang), jnp.sin(ang)


def _ksq():
    kx = jnp.arange(KX, dtype=jnp.int32)
    k = jnp.arange(N, dtype=jnp.int32)
    k = jnp.where(k <= N // 2, k, k - N)
    k2 = kx[:, None, None] ** 2 + k[None, :, None] ** 2 + k[None, None, :] ** 2
    return k2.astype(jnp.float32)


def setup_inputs(seed: int = 0) -> dict:
    k1, k2 = jax.random.split(jax.random.key(seed))
    u = jax.random.normal(k1, (N, N, N), jnp.float32)
    r = jax.random.uniform(k2, (KX, N, N), jnp.float32, -1.0, 1.0)
    g = (1.0 + 0.5 * r) / (1.0 + _ksq() / (N / 4.0) ** 2)
    g = g / jnp.sqrt(jnp.mean(g[: N // 2 + 1] ** 2))
    return {"u": u, "g": g.astype(jnp.float32)}


def _line(xr, xi, c, s, form, sign):
    f = lambda p, q: jnp.einsum(form, p.astype(jnp.float32), q.astype(jnp.float32), precision=HI)
    return f(xr, c) + sign * f(xi, s), f(xi, c) - sign * f(xr, s)


def reference(u, g):
    c, s = _trig(N, N)
    cx, sx = _trig(KX, N)
    k = jnp.arange(KX)
    keep = (k <= N // 2).astype(jnp.float32)
    wgt = jnp.where((k == 0) | (k == N // 2), 1.0, 2.0) * keep / N
    u2 = u.reshape(N, N * N)
    xr = jnp.dot(cx * keep[:, None], u2, precision=HI, preferred_element_type=jnp.float32).reshape(KX, N, N)
    xi = jnp.dot(-sx * keep[:, None], u2, precision=HI, preferred_element_type=jnp.float32).reshape(KX, N, N)
    xr, xi = _line(xr, xi, c, s, "xyz,yk->xkz", 1.0)
    xr, xi = _line(xr, xi, c, s, "xyz,zk->xyk", 1.0)
    xr, xi = xr * g, xi * g
    xr, xi = _line(xr, xi, c / N, s / N, "xyz,zk->xyk", -1.0)
    xr, xi = _line(xr, xi, c / N, s / N, "xyz,yk->xkz", -1.0)
    ar = (cx * wgt[:, None]).T
    ai = (sx * wgt[:, None]).T
    w = jnp.dot(ar, xr.reshape(KX, N * N), precision=HI, preferred_element_type=jnp.float32) - jnp.dot(ai, xi.reshape(KX, N * N), precision=HI, preferred_element_type=jnp.float32)
    return w.reshape(N, N, N)
```

```python
import functools
import math
import numpy as np
import jax
import jax.numpy as jnp
from jax import lax
from jax.experimental import pallas as pl
from jax.experimental.pallas import tpu as pltpu
from jax.sharding import PartitionSpec as P

HI = lax.Precision.HIGHEST
MESH = pl.DeviceIdType.MESH
F32 = jnp.float32
KC = 2


def _trig(n, rows, cols):
    r = np.arange(rows)[:, None]
    c = np.arange(cols)[None, :]
    ang = ((r * c) % n).astype(np.float32) * np.float32(2.0 * math.pi / n)
    ang = ang.astype(np.float64)
    return np.cos(ang).astype(np.float32), np.sin(ang).astype(np.float32)


def _tables(n, kx, nb):
    cx, sx = _trig(n, kx, n)
    k = np.arange(kx)
    keep = (k <= n // 2).astype(np.float32)[:, None]
    wgt = np.where((k == 0) | (k == n // 2), 1.0, 2.0).astype(np.float32)[:, None] * keep / np.float32(n)
    tx = np.concatenate([cx * keep, -sx * keep], axis=0)
    txi = np.concatenate([cx * wgt, -sx * wgt], axis=0)
    c, s = _trig(n, n, n)
    ty = np.concatenate([c, s], axis=0)
    zb = n // nb
    rows = []
    for b in range(nb):
        cb, sb = c[b * zb:(b + 1) * zb], s[b * zb:(b + 1) * zb]
        rows += [np.concatenate([cb, -sb], axis=1), np.concatenate([sb, cb], axis=1)]
    tz = np.concatenate(rows, axis=0)
    return [np.ascontiguousarray(t, dtype=np.float32) for t in (tx, txi, ty, tz)]


def _dot(p, q, dims=((1,), (0,))):
    return lax.dot_general(p, q, (dims, ((), ())), precision=HI, preferred_element_type=F32)


def _kernel(n, na, nb, kl, u_hbm, g_hbm, tx_hbm, txi_hbm, ty_hbm, tz_hbm, w_hbm,
            u, g, tx, txi, ty, tz, xs, ai, yf, bi, bo, vi, iy, ao, w,
            lsem, usem, wsem, ssem, ra, rb, rbo, rao):
    a, b = lax.axis_index("a"), lax.axis_index("b")
    ya, zb = n // na, n // nb
    kx = na * kl
    rows = 4 * zb
    nj = ya * zb // rows
    full, rest = kl // KC, kl % KC

    def local(src, dst, sem):
        return pltpu.make_async_copy(src, dst, sem)

    load_u = [local(u_hbm.at[pl.ds(j * rows, rows)], u.at[pl.ds(j * rows, rows)], usem.at[j]) for j in range(nj)]
    loads = [local(s, d, lsem.at[i]) for i, (s, d) in enumerate(
        [(tx_hbm, tx), (ty_hbm, ty), (tz_hbm, tz), (g_hbm, g), (txi_hbm, txi)])]
    loads[0].start()
    for cp in load_u:
        cp.start()
    for cp in loads[1:]:
        cp.start()

    bar = pltpu.get_barrier_semaphore()
    for d in range(1, na):
        pl.semaphore_signal(bar, inc=1, device_id=(b, lax.rem(a + d, na)), device_id_type=MESH)
    for d in range(1, nb):
        pl.semaphore_signal(bar, inc=1, device_id=(lax.rem(b + d, nb), a), device_id_type=MESH)
    pl.semaphore_wait(bar, na + nb - 2)

    def lanes(shape):
        return lax.broadcasted_iota(jnp.int32, shape, 1) < zb

    xs2 = xs.reshape(kx * ya, 2 * zb)
    ao2 = ao.reshape(kx * ya, 2 * zb)

    loads[0].wait()

    def xfwd(j, _):
        local(u_hbm.at[pl.ds(j * rows, rows)], u.at[pl.ds(j * rows, rows)], usem.at[j]).wait()
        r = _dot(tx[...], u[pl.ds(pl.multiple_of(j * rows, rows), rows), :], ((1,), (1,)))
        lo = lanes((kx, 2 * zb))
        for h in range(2):
            re = r[:kx, 2 * zb * h:2 * zb * (h + 1)]
            im = r[kx:, 2 * zb * h:2 * zb * (h + 1)]
            y = 4 * j + 2 * h
            xs2[pl.ds(y, kx, stride=ya), :] = jnp.where(lo, re, pltpu.roll(im, zb, 1))
            xs2[pl.ds(y + 1, kx, stride=ya), :] = jnp.where(lo, pltpu.roll(re, zb, 1), im)
        return 0

    lax.fori_loop(0, nj, xfwd, 0)

    def chunks(step):
        def body(c, _):
            step(c, c * KC, KC)
            return 0
        lax.fori_loop(0, full, body, 0)
        if rest:
            step(full, full * KC, rest)

    def send_a(c, k, kc):
        for d in range(1, na):
            t = lax.rem(a + d, na)
            pltpu.make_async_remote_copy(
                xs.at[pl.ds(t * kl + k, kc)], ai.at[pl.ds(k, kc), pl.ds(a * ya, ya)],
                ssem.at[0], ra.at[c], device_id=(b, t), device_id_type=MESH).start()
        local(xs.at[pl.ds(a * kl + k, kc)], ai.at[pl.ds(k, kc), pl.ds(a * ya, ya)], ra.at[c]).start()

    chunks(send_a)
    loads[1].wait()

    def ydft(src, dst, k, kc, scale, sign):
        x = jnp.concatenate([src[k + i] for i in range(kc)], axis=1)
        if scale is not None:
            x = x * scale
        r = _dot(ty[...], x)
        lo = lanes((n, 2 * zb))
        for i in range(kc):
            p = r[:n, 2 * zb * i:2 * zb * (i + 1)]
            q = pltpu.roll(r[n:, 2 * zb * i:2 * zb * (i + 1)], zb, 1)
            dst[k + i] = p + jnp.where(lo, sign * q, -sign * q)

    def yfwd(c, k, kc):
        blk = ai.at[pl.ds(k, kc)]
        local(blk, blk, ra.at[c]).wait()
        ydft(ai, yf, k, kc, None, 1.0)
        for d in range(1, nb):
            t = lax.rem(b + d, nb)
            pltpu.make_async_remote_copy(
                yf.at[pl.ds(k, kc), pl.ds(t * zb, zb)], bi.at[pl.ds(k, kc), :, pl.ds(b * 2 * zb, 2 * zb)],
                ssem.at[1], rb.at[c], device_id=(t, a), device_id_type=MESH).start()
        local(yf.at[pl.ds(k, kc), pl.ds(b * zb, zb)], bi.at[pl.ds(k, kc), :, pl.ds(b * 2 * zb, 2 * zb)], rb.at[c]).start()

    chunks(yfwd)
    loads[2].wait()
    loads[3].wait()

    def zfilt(c, k, kc):
        blk = bi.at[pl.ds(k, kc)]
        local(blk, blk, rb.at[c]).wait()
        x = bi[pl.ds(k, kc)].reshape(kc * zb, 2 * n)
        f = _dot(x, tz[...])
        gg = g[pl.ds(k, kc)].reshape(kc * zb, n)
        v = f * jnp.concatenate([gg, gg], axis=1) * (1.0 / n)
        o = _dot(v, tz[...], ((1,), (1,)))
        bo[pl.ds(k, kc)] = o.reshape(kc, zb, 2 * n)
        for d in range(1, nb):
            t = lax.rem(b + d, nb)
            pltpu.make_async_remote_copy(
                bo.at[pl.ds(k, kc), :, pl.ds(t * 2 * zb, 2 * zb)], vi.at[pl.ds(k, kc), pl.ds(b * zb, zb)],
                ssem.at[2], rbo.at[c], device_id=(t, a), device_id_type=MESH).start()
        local(bo.at[pl.ds(k, kc), :, pl.ds(b * 2 * zb, 2 * zb)], vi.at[pl.ds(k, kc), pl.ds(b * zb, zb)], rbo.at[c]).start()

    chunks(zfilt)

    def yinv(c, k, kc):
        blk = vi.at[pl.ds(k, kc)]
        local(blk, blk, rbo.at[c]).wait()
        ydft(vi, iy, k, kc, 1.0 / n, -1.0)
        for d in range(1, na):
            t = lax.rem(a + d, na)
            pltpu.make_async_remote_copy(
                iy.at[pl.ds(k, kc), pl.ds(t * ya, ya)], ao.at[pl.ds(a * kl + k, kc)],
                ssem.at[3], rao.at[c], device_id=(b, t), device_id_type=MESH).start()
        local(iy.at[pl.ds(k, kc), pl.ds(a * ya, ya)], ao.at[pl.ds(a * kl + k, kc)], rao.at[c]).start()

    chunks(yinv)
    loads[4].wait()

    def wait_ao(c, k, kc):
        blk = ao.at[pl.ds(0, na * kc)]
        local(blk, blk, rao.at[c]).wait()

    chunks(wait_ao)

    def xinv(j, _):
        lo = lanes((kx, 2 * zb))
        parts = []
        for h in range(2):
            y = 4 * j + 2 * h
            p = ao2[pl.ds(y, kx, stride=ya), :]
            q = ao2[pl.ds(y + 1, kx, stride=ya), :]
            re = jnp.where(lo, p, pltpu.roll(q, zb, 1))
            im = jnp.where(lo, pltpu.roll(p, zb, 1), q)
            parts.append(jnp.concatenate([re, im], axis=0))
        d = jnp.concatenate(parts, axis=1)
        at = pl.ds(pl.multiple_of(j * rows, rows), rows)
        w[at, :] = _dot(d, txi[...], ((0,), (0,)))
        local(w.at[at], w_hbm.at[at], wsem).start()
        return 0

    lax.fori_loop(0, nj, xinv, 0)
    local(w, w_hbm, wsem).wait()
    sa = xs.at[pl.ds(0, (na - 1) * kl)]
    sb = yf.at[:, pl.ds(0, (nb - 1) * zb)]
    local(sa, sa, ssem.at[0]).wait()
    local(sb, sb, ssem.at[1]).wait()
    local(sb, sb, ssem.at[2]).wait()
    local(sa, sa, ssem.at[3]).wait()


def solution(mesh):
    na, nb = mesh.shape["a"], mesh.shape["b"]

    def body(u, g):
        n, ya, zb = u.shape
        kl = g.shape[0]
        kx = kl * na
        tabs = _tables(n, kx, nb)
        ut = jnp.transpose(u, (1, 2, 0)).reshape(ya * zb, n)
        nchunk = -(-kl // KC)
        nj = ya // 4
        vm = lambda *s: pltpu.VMEM(s, F32)
        dma = lambda *s: pltpu.SemaphoreType.DMA(s)
        hbm = pl.BlockSpec(memory_space=pl.ANY)
        w = pl.pallas_call(
            functools.partial(_kernel, n, na, nb, kl),
            name="fftfilter",
            out_shape=jax.ShapeDtypeStruct((ya * zb, n), F32),
            in_specs=[hbm] * 6,
            out_specs=hbm,
            scratch_shapes=[
                vm(ya * zb, n), vm(kl, zb, n), vm(*tabs[0].shape), vm(*tabs[1].shape), vm(*tabs[2].shape), vm(*tabs[3].shape),
                vm(kx, ya, 2 * zb), vm(kl, n, 2 * zb), vm(kl, n, 2 * zb), vm(kl, zb, 2 * n), vm(kl, zb, 2 * n),
                vm(kl, n, 2 * zb), vm(kl, n, 2 * zb), vm(kx, ya, 2 * zb), vm(ya * zb, n),
                dma(5), dma(nj), pltpu.SemaphoreType.DMA, dma(4), dma(nchunk), dma(nchunk), dma(nchunk), dma(nchunk),
            ],
            compiler_params=pltpu.CompilerParams(
                collective_id=0, has_side_effects=True, vmem_limit_bytes=60000 * 1024),
        )(ut, g, *[jnp.asarray(t) for t in tabs])
        return jnp.transpose(w.reshape(ya, zb, n), (2, 0, 1))

    return jax.shard_map(body, mesh=mesh, in_specs=(P(None, "a", "b"), P("a", "b", None)),
                         out_specs=P(None, "a", "b"), check_vma=False)
```

```python
import functools
import math
import numpy as np
import jax
import jax.numpy as jnp
from jax import lax
from jax.experimental import pallas as pl
from jax.experimental.pallas import tpu as pltpu
from jax.sharding import PartitionSpec as P

HI = lax.Precision.HIGHEST
MESH = pl.DeviceIdType.MESH
F32 = jnp.float32
KC = 2
GC = 2
LZ = 2
LY = 4
TX = 5
PX = 2
NP = 4


def _trig(n, rows, cols):
    r = np.arange(rows)[:, None]
    c = np.arange(cols)[None, :]
    ang = ((r * c) % n).astype(np.float32) * np.float32(2.0 * math.pi / n)
    ang = ang.astype(np.float64)
    return np.cos(ang).astype(np.float32), np.sin(ang).astype(np.float32)


def _plan(n, na, kl):
    modes = n // 2 + 1
    slots = kl - 1
    own = modes - kl * (na - 1)
    assert own + na - 2 == slots and slots % KC == 0
    kx = kl * np.arange(na)[:, None] + np.arange(slots)[None, :]
    kx[na - 1, own:] = kl * np.arange(na - 2) + slots
    return kx, kl * (na - 2) + slots, own


def _tables(n, na, nb, kl):
    kx, extra, _ = _plan(n, na, kl)
    pad = (-(kx.size + 1)) % 8
    c, s = _trig(n, n, n)

    def rows(t, k):
        return np.concatenate([t[k.reshape(-1)], t[[extra]], np.zeros((pad, n), np.float32)])

    tx = np.concatenate([rows(c, kx), rows(-s, kx)])
    wgt = np.where((np.arange(n) == 0) | (np.arange(n) == n // 2), 1.0, 2.0).astype(np.float32)[:, None] / np.float32(n)
    wc, ws = c * wgt, -s * wgt
    txi = []
    z7 = np.zeros((7, n), np.float32)
    for p, k in enumerate(range(0, kx.shape[1], KC * GC)):
        sel = kx[:, k:k + KC * GC].T.reshape(-1)
        txi += [wc[sel], ws[sel]]
        if p == PX:
            txi += [wc[[extra]], z7, ws[[extra]], z7]
    ty = np.concatenate([c, s], axis=0)
    zb = n // nb
    tz = []
    for b in range(nb):
        cb, sb = c[b * zb:(b + 1) * zb], s[b * zb:(b + 1) * zb]
        tz += [np.concatenate([cb, -sb], axis=1), np.concatenate([sb, cb], axis=1)]
    return [np.ascontiguousarray(t, dtype=np.float32) for t in (tx, np.concatenate(txi), ty, np.concatenate(tz))]


def _dot(p, q, dims=((1,), (0,))):
    return lax.dot_general(p, q, (dims, ((), ())), precision=HI, preferred_element_type=F32)


def _kernel(n, na, nb, kl, own, u_hbm, g_hbm, tx_hbm, txi_hbm, ty_hbm, tz_hbm, w_hbm,
            u, g, tx, txi, ty, tz, xs, ai, yf, bi, bo, vi, iy, ao, aox, w,
            lsem, usem, wsem, ssem, ra, rb, rbo, rao, rg):
    a, b = lax.axis_index("a"), lax.axis_index("b")
    ya, zb = n // na, n // nb
    slots = kl - 1
    nk = slots // KC
    kx = xs.shape[0]
    xrow = na * slots
    ex = na - 2
    rows = 4 * zb
    nj = ya * zb // rows
    lane = 2 * zb

    def local(src, dst, sem):
        return pltpu.make_async_copy(src, dst, sem)

    def remote(src, dst, s, r, t):
        return pltpu.make_async_remote_copy(src, dst, s, r, device_id=t, device_id_type=MESH)

    def wait(ref, sem):
        local(ref, ref, sem).wait()

    bar = pltpu.get_barrier_semaphore()
    for d in range(1, na):
        pl.semaphore_signal(bar, inc=1, device_id=(b, lax.rem(a + d, na)), device_id_type=MESH)
    for d in range(1, nb):
        pl.semaphore_signal(bar, inc=1, device_id=(lax.rem(b + d, nb), a), device_id_type=MESH)

    def load_u(j):
        at = pl.ds(pl.multiple_of(j * rows, rows), rows)
        return local(u_hbm.at[at], u.at[at], usem.at[j])

    loads = [local(s, d, lsem.at[i]) for i, (s, d) in enumerate(
        [(tx_hbm, tx), (ty_hbm, ty), (tz_hbm, tz), (txi_hbm, txi), (g_hbm.at[pl.ds(0, own)], g.at[pl.ds(0, own)])])]
    load_g = local(g_hbm.at[pl.ds(own, kl - own)], g.at[pl.ds(own, kl - own)], lsem.at[5])
    loads[0].start()
    for j in range(nj):
        load_u(j).start()
    for cp in loads[1:]:
        cp.start()

    @pl.when(a < na - 1)
    def _():
        load_g.start()

    def lanes(shape):
        return lax.broadcasted_iota(jnp.int32, shape, 1) < zb

    xs2 = xs.reshape(kx * ya, lane)

    def send_a(c, k, kc, y, yc):
        for d in range(1, na):
            t = lax.rem(a + d, na)
            remote(xs.at[pl.ds(t * slots + k, kc), pl.ds(y, yc)], ai.at[pl.ds(k, kc), pl.ds(a * ya + y, yc)],
                   ssem.at[0], ra.at[c], (b, t)).start()
        local(xs.at[pl.ds(a * slots + k, kc), pl.ds(y, yc)], ai.at[pl.ds(k, kc), pl.ds(a * ya + y, yc)], ra.at[c]).start()

    loads[0].wait()

    def xfwd(j, _):
        load_u(j).wait()
        r = _dot(tx[...], u[pl.ds(pl.multiple_of(j * rows, rows), rows), :], ((1,), (1,)))
        lo = lanes((kx, lane))
        for h in range(2):
            re = r[:kx, lane * h:lane * (h + 1)]
            im = r[kx:, lane * h:lane * (h + 1)]
            y = 4 * j + 2 * h
            xs2[pl.ds(y, kx, stride=ya), :] = jnp.where(lo, re, pltpu.roll(im, zb, 1))
            xs2[pl.ds(y + 1, kx, stride=ya), :] = jnp.where(lo, pltpu.roll(re, zb, 1), im)
        return 0

    lax.fori_loop(0, nj // 2, xfwd, 0)
    pl.semaphore_wait(bar, na + nb - 2)
    send_a(0, 0, KC, 0, ya // 2)
    lax.fori_loop(nj // 2, 3 * nj // 4, xfwd, 0)
    send_a(0, 0, KC, ya // 2, ya // 4)
    lax.fori_loop(3 * nj // 4, nj, xfwd, 0)
    send_a(0, 0, KC, 3 * ya // 4, ya // 4)

    def rest_a(c, _):
        send_a(c, c * KC, KC, 0, ya)
        return 0

    lax.fori_loop(1, nk, rest_a, 0)
    xsx, aix = xs.at[pl.ds(xrow, 1)], ai.at[pl.ds(slots, 1), pl.ds(a * ya, ya)]
    to_ex = remote(xsx, aix, ssem.at[4], ra.at[nk], (b, ex))
    to_me = local(xsx, aix, ra.at[nk])
    send_g = remote(g_hbm.at[slots], g.at[own + a], ssem.at[8], rg, (b, na - 1))

    @pl.when(a != ex)
    def _():
        to_ex.start()

    @pl.when(a == ex)
    def _():
        to_me.start()

    @pl.when(a < ex)
    def _():
        send_g.start()

    w[...] = jnp.zeros_like(w)
    aox[...] = jnp.zeros_like(aox)
    loads[1].wait()

    def ydft(src, dst, k, kc, scale, sign):
        x = jnp.concatenate([src[k + i] for i in range(kc)], axis=1)
        if scale is not None:
            x = x * scale
        r = _dot(ty[...], x)
        lo = lanes((n, lane))
        for i in range(kc):
            p = r[:n, lane * i:lane * (i + 1)]
            q = pltpu.roll(r[n:, lane * i:lane * (i + 1)], zb, 1)
            dst[k + i] = p + jnp.where(lo, sign * q, -sign * q)

    def yfwd(c, k, kc, s):
        wait(ai.at[pl.ds(k, kc)], ra.at[c])
        ydft(ai, yf, k, kc, None, 1.0)
        for d in range(1, nb):
            t = lax.rem(b + d, nb)
            remote(yf.at[pl.ds(k, kc), pl.ds(t * zb, zb)], bi.at[pl.ds(k, kc), :, pl.ds(b * lane, lane)],
                   s, rb.at[c], (t, a)).start()
        local(yf.at[pl.ds(k, kc), pl.ds(b * zb, zb)], bi.at[pl.ds(k, kc), :, pl.ds(b * lane, lane)], rb.at[c]).start()

    def zfilt(c, k, kc, s):
        wait(bi.at[pl.ds(k, kc)], rb.at[c])
        x = bi[pl.ds(k, kc)].reshape(kc * zb, 2 * n)
        f = _dot(x, tz[...])
        gg = g[pl.ds(k, kc)].reshape(kc * zb, n)
        v = f * jnp.concatenate([gg, gg], axis=1) * (1.0 / n)
        o = _dot(v, tz[...], ((1,), (1,)))
        bo[pl.ds(k, kc)] = o.reshape(kc, zb, 2 * n)
        for d in range(1, nb):
            t = lax.rem(b + d, nb)
            remote(bo.at[pl.ds(k, kc), :, pl.ds(t * lane, lane)], vi.at[pl.ds(k, kc), pl.ds(b * zb, zb)],
                   s, rbo.at[c if kc > 1 else nk - 1 + NP], (t, a)).start()
        local(bo.at[pl.ds(k, kc), :, pl.ds(b * lane, lane)], vi.at[pl.ds(k, kc), pl.ds(b * zb, zb)], rbo.at[c if kc > 1 else nk - 1 + NP]).start()

    def yinv(c, k, kc, s, pieces=1):
        wait(vi.at[pl.ds(k, kc)], rbo.at[c])
        ydft(vi, iy, k, kc, 1.0 / n, -1.0)
        yc = ya // pieces
        for p in range(pieces):
            dst = aox.at[pl.ds(0, 1)] if kc == 1 else ao.at[pl.ds(k, kc), a, pl.ds(p * yc, yc)]
            for d in range(1, na):
                t = lax.rem(a + d, na)
                remote(iy.at[pl.ds(k, kc), pl.ds(t * ya + p * yc, yc)], dst, s, rao.at[c + p], (b, t)).start()
            local(iy.at[pl.ds(k, kc), pl.ds(a * ya + p * yc, yc)], dst, rao.at[c + p]).start()

    ao2 = ao.reshape(slots * na * ya, lane)
    aox2 = aox.reshape(8 * ya, lane)
    m = GC * KC * na
    ly = 8

    def xinv(p, last):
        extra = p == PX
        trow = 2 * m * p + (16 if p > PX else 0)
        table = txi[trow:trow + 2 * m + (16 if extra else 0), :]
        srcs = [(ao2, p * m * ya, m)] + ([(aox2, 0, 8)] if extra else [])

        def body(j, _):
            if last:
                pc = j * ly // (ya // NP)

                @pl.when(j * ly % (ya // NP) == 0)
                def _():
                    wait(ao.at[pl.ds(0, KC), :, pl.ds(0, ya // NP)], rao.at[nk - 1 + pc])
            cols = []
            for h in range(ly // 2):
                parts = []
                for src, first, r in srcs:
                    lo = lanes((r, lane))
                    y = first + ly * j + 2 * h
                    f = src[pl.ds(y, r, stride=ya), :]
                    q = src[pl.ds(y + 1, r, stride=ya), :]
                    parts += [jnp.where(lo, f, pltpu.roll(q, zb, 1)), jnp.where(lo, pltpu.roll(f, zb, 1), q)]
                cols.append(jnp.concatenate(parts, axis=0))
            at = pl.ds(pl.multiple_of(j * (ly * zb), ly * zb), ly * zb)
            w[at, :] += _dot(jnp.concatenate(cols, axis=1), table, ((0,), (0,)))
            if last:
                local(w.at[at], w_hbm.at[at], wsem).start()
            return 0

        for c in range(GC * p, GC * (p + 1) - (1 if last else 0)):
            wait(ao.at[pl.ds(0, KC)], rao.at[c])
        if extra:
            wait(aox.at[0], rao.at[nk - 1 + NP])
        lax.fori_loop(0, ya // ly, body, 0)

    def step(t, _):
        @pl.when(t < nk)
        def _():
            yfwd(t, t * KC, KC, ssem.at[1])

        @pl.when((t == TX) & (a == ex))
        def _():
            yfwd(nk, slots, 1, ssem.at[5])

        @pl.when(t == LZ)
        def _():
            for i in (2, 4):
                loads[i].wait()

            @pl.when(a < na - 1)
            def _():
                load_g.wait()

        @pl.when((t == LZ + own // KC) & (a == na - 1))
        def _():
            wait(g.at[pl.ds(own, ex)], rg)

        @pl.when((t >= LZ) & (t < nk + LZ))
        def _():
            zfilt(t - LZ, (t - LZ) * KC, KC, ssem.at[2])

        @pl.when((t == TX + LZ) & (a == ex))
        def _():
            zfilt(nk, slots, 1, ssem.at[6])

        @pl.when(t >= LY)
        def _():
            yinv(t - LY, (t - LY) * KC, KC, ssem.at[3])

        @pl.when((t == TX + LY) & (a == ex))
        def _():
            yinv(nk - 1 + NP, slots, 1, ssem.at[7])

        for p in range(nk // GC - 2):
            @pl.when(t == GC * (p + 1) + LY)
            def _():
                if p == 0:
                    loads[3].wait()
                xinv(p, False)
        return 0

    lax.fori_loop(0, nk + LY - 1, step, 0)
    yinv(nk - 1, (nk - 1) * KC, KC, ssem.at[3], NP)
    xinv(nk // GC - 2, False)
    xinv(nk // GC - 1, True)
    wait_w = local(w, w_hbm, wsem)
    wait_w.wait()

    sa = xs.at[pl.ds(0, (na - 1) * slots)]
    sb = yf.at[pl.ds(0, slots), pl.ds(0, (nb - 1) * zb)]
    wait(sa, ssem.at[0])
    wait(sb, ssem.at[1])
    wait(sb, ssem.at[2])
    wait(sa, ssem.at[3])

    @pl.when(a != ex)
    def _():
        wait(xs.at[0], ssem.at[4])

    @pl.when(a == ex)
    def _():
        wait(yf.at[0, pl.ds(0, (nb - 1) * zb)], ssem.at[5])
        wait(yf.at[0, pl.ds(0, (nb - 1) * zb)], ssem.at[6])
        wait(xs.at[pl.ds(0, na - 1)], ssem.at[7])

    @pl.when(a < ex)
    def _():
        wait(g.at[0], ssem.at[8])


def solution(mesh):
    na, nb = mesh.shape["a"], mesh.shape["b"]

    def body(u, g):
        n, ya, zb = u.shape
        kl = g.shape[0]
        own = _plan(n, na, kl)[2]
        tabs = _tables(n, na, nb, kl)
        ut = jnp.transpose(u, (1, 2, 0)).reshape(ya * zb, n)
        nk = (kl - 1) // KC
        vm = lambda *s: pltpu.VMEM(s, F32)
        dma = lambda *s: pltpu.SemaphoreType.DMA(s)
        hbm = pl.BlockSpec(memory_space=pl.ANY)
        w = pl.pallas_call(
            functools.partial(_kernel, n, na, nb, kl, own),
            name="fftfilter",
            out_shape=jax.ShapeDtypeStruct((ya * zb, n), F32),
            in_specs=[hbm] * 6,
            out_specs=hbm,
            scratch_shapes=[
                vm(ya * zb, n), vm(kl, zb, n), *[vm(*t.shape) for t in tabs],
                vm(tabs[0].shape[0] // 2, ya, 2 * zb), vm(kl, n, 2 * zb), vm(kl, n, 2 * zb),
                vm(kl, zb, 2 * n), vm(kl, zb, 2 * n), vm(kl, n, 2 * zb), vm(kl, n, 2 * zb),
                vm(kl - 1, na, ya, 2 * zb), vm(8, ya, 2 * zb), vm(ya * zb, n),
                dma(6), dma(ya // 4), pltpu.SemaphoreType.DMA, dma(9),
                dma(nk + 1), dma(nk + 1), dma(nk + NP), dma(nk + NP), pltpu.SemaphoreType.DMA,
            ],
            compiler_params=pltpu.CompilerParams(
                collective_id=0, has_side_effects=True, vmem_limit_bytes=60000 * 1024),
        )(ut, g, *[jnp.asarray(t) for t in tabs])
        return jnp.transpose(w.reshape(ya, zb, n), (2, 0, 1))

    return jax.shard_map(body, mesh=mesh, in_specs=(P(None, "a", "b"), P("a", "b", None)),
                         out_specs=P(None, "a", "b"), check_vma=False)
```

```python
import functools
import math
import numpy as np
import jax
import jax.numpy as jnp
from jax import lax
from jax.experimental import pallas as pl
from jax.experimental.pallas import tpu as pltpu
from jax.sharding import PartitionSpec as P

HI = lax.Precision.HIGHEST
MESH = pl.DeviceIdType.MESH
F32 = jnp.float32
KC = 2
GC = 4
LZ = 2
LY = 4
TX = 5
PX = 1
NP = 4


def _trig(n, rows, cols):
    r = np.arange(rows)[:, None]
    c = np.arange(cols)[None, :]
    ang = ((r * c) % n).astype(np.float32) * np.float32(2.0 * math.pi / n)
    ang = ang.astype(np.float64)
    return np.cos(ang).astype(np.float32), np.sin(ang).astype(np.float32)


def _plan(n, na, kl):
    modes = n // 2 + 1
    slots = kl - 1
    own = modes - kl * (na - 1)
    assert own + na - 2 == slots and slots % KC == 0
    kx = kl * np.arange(na)[:, None] + np.arange(slots)[None, :]
    kx[na - 1, own:] = kl * np.arange(na - 2) + slots
    return kx, kl * (na - 2) + slots, own


def _tables(n, na, nb, kl):
    kx, extra, _ = _plan(n, na, kl)
    pad = (-(kx.size + 1)) % 8
    c, s = _trig(n, n, n)

    def rows(t, k):
        return np.concatenate([t[k.reshape(-1)], t[[extra]], np.zeros((pad, n), np.float32)])

    tx = np.concatenate([rows(c, kx), rows(-s, kx)])
    wgt = np.where((np.arange(n) == 0) | (np.arange(n) == n // 2), 1.0, 2.0).astype(np.float32)[:, None] / np.float32(n)
    wc, ws = c * wgt, -s * wgt
    txi = []
    z7 = np.zeros((7, n), np.float32)
    for p, k in enumerate(range(0, kx.shape[1], KC * GC)):
        sel = kx[:, k:k + KC * GC].T.reshape(-1)
        txi += [wc[sel], ws[sel]]
        if p == PX:
            txi += [wc[[extra]], z7, ws[[extra]], z7]
    ty = np.concatenate([c, s], axis=0)
    zb = n // nb
    tz = []
    for b in range(nb):
        cb, sb = c[b * zb:(b + 1) * zb], s[b * zb:(b + 1) * zb]
        tz += [np.concatenate([cb, -sb], axis=1), np.concatenate([sb, cb], axis=1)]
    tz = np.concatenate(tz, axis=0)
    return [np.ascontiguousarray(t, dtype=np.float32) for t in (tx, np.concatenate(txi), ty, tz[:, :n], tz[:, n:])]


def _dot(p, q, dims=((1,), (0,))):
    return lax.dot_general(p, q, (dims, ((), ())), precision=HI, preferred_element_type=F32)


def _kernel(n, na, nb, kl, own, u_hbm, g_hbm, tab_hbm, *refs):
    out, refs = refs[:n // na // 8], refs[n // na // 8:]
    (u, g, tx, txi, ty, tz, xs, ai, yf, bi, bo, vi, iy, ao, aox, w,
            lsem, usem, ssem, ra, rb, rbo, rao, rg) = refs
    a, b = lax.axis_index("a"), lax.axis_index("b")
    ya, zb = n // na, n // nb
    slots = kl - 1
    nk = slots // KC
    kx = xs.shape[0]
    xrow = na * slots
    ex = na - 2
    rows = 4 * zb
    nj = ya * zb // rows
    lane = 2 * zb

    def local(src, dst, sem):
        return pltpu.make_async_copy(src, dst, sem)

    def remote(src, dst, s, r, t):
        return pltpu.make_async_remote_copy(src, dst, s, r, device_id=t, device_id_type=MESH)

    def wait(ref, sem):
        local(ref, ref, sem).wait()

    bar = pltpu.get_barrier_semaphore()
    for d in range(1, na):
        pl.semaphore_signal(bar, inc=1, device_id=(b, lax.rem(a + d, na)), device_id_type=MESH)
    for d in range(1, nb):
        pl.semaphore_signal(bar, inc=1, device_id=(lax.rem(b + d, nb), a), device_id_type=MESH)

    def load_u(j):
        at = pl.ds(pl.multiple_of(j * rows, rows), rows)
        return local(u_hbm.at[at], u.at[at], usem.at[j])

    loads, at = [], 0
    for d in (tx, txi, ty, tz.at[:, pl.ds(0, n)], tz.at[:, pl.ds(n, n)]):
        loads.append(local(tab_hbm.at[pl.ds(at, d.shape[0])], d, lsem.at[len(loads)]))
        at += d.shape[0]
    loads.append(local(g_hbm.at[pl.ds(0, own)], g.at[pl.ds(0, own)], lsem.at[5]))
    load_g = local(g_hbm.at[pl.ds(own, kl - own)], g.at[pl.ds(own, kl - own)], lsem.at[6])
    loads[0].start()
    for j in range(nj):
        load_u(j).start()
    for cp in loads[1:]:
        cp.start()

    @pl.when(a < na - 1)
    def _():
        load_g.start()

    def lanes(shape):
        return lax.broadcasted_iota(jnp.int32, shape, 1) < zb

    xs2 = xs.reshape(kx * ya, lane)

    def send_a(c, k, kc, y, yc):
        for d in range(1, na):
            t = lax.rem(a + d, na)
            remote(xs.at[pl.ds(t * slots + k, kc), pl.ds(y, yc)], ai.at[pl.ds(k, kc), pl.ds(a * ya + y, yc)],
                   ssem.at[0], ra.at[c], (b, t)).start()
        local(xs.at[pl.ds(a * slots + k, kc), pl.ds(y, yc)], ai.at[pl.ds(k, kc), pl.ds(a * ya + y, yc)], ra.at[c]).start()

    loads[0].wait()

    def xfwd(j, _):
        load_u(j).wait()
        r = _dot(tx[...], u[pl.ds(pl.multiple_of(j * rows, rows), rows), :], ((1,), (1,)))
        lo = lanes((kx, lane))
        for h in range(2):
            re = r[:kx, lane * h:lane * (h + 1)]
            im = r[kx:, lane * h:lane * (h + 1)]
            y = 4 * j + 2 * h
            xs2[pl.ds(y, kx, stride=ya), :] = jnp.where(lo, re, pltpu.roll(im, zb, 1))
            xs2[pl.ds(y + 1, kx, stride=ya), :] = jnp.where(lo, pltpu.roll(re, zb, 1), im)
        return 0

    lax.fori_loop(0, nj // 2, xfwd, 0)
    pl.semaphore_wait(bar, na + nb - 2)
    send_a(0, 0, KC, 0, ya // 2)
    lax.fori_loop(nj // 2, 3 * nj // 4, xfwd, 0)
    send_a(0, 0, KC, ya // 2, ya // 4)
    lax.fori_loop(3 * nj // 4, nj, xfwd, 0)
    send_a(0, 0, KC, 3 * ya // 4, ya // 4)

    send_a(1, KC, KC, 0, ya)
    w[...] = jnp.zeros_like(w)
    aox[...] = jnp.zeros_like(aox)
    loads[2].wait()

    def ydft(src, dst, k, kc, scale, sign):
        x = jnp.concatenate([src[k + i] for i in range(kc)], axis=1)
        if scale is not None:
            x = x * scale
        r = _dot(ty[...], x)
        lo = lanes((n, lane))
        for i in range(kc):
            p = r[:n, lane * i:lane * (i + 1)]
            q = pltpu.roll(r[n:, lane * i:lane * (i + 1)], zb, 1)
            dst[k + i] = p + jnp.where(lo, sign * q, -sign * q)

    def yfwd(c, k, kc, s):
        wait(ai.at[pl.ds(k, kc)], ra.at[c])
        ydft(ai, yf, k, kc, None, 1.0)
        for d in range(1, nb):
            t = lax.rem(b + d, nb)
            remote(yf.at[pl.ds(k, kc), pl.ds(t * zb, zb)], bi.at[pl.ds(k, kc), :, pl.ds(b * lane, lane)],
                   s, rb.at[c], (t, a)).start()
        local(yf.at[pl.ds(k, kc), pl.ds(b * zb, zb)], bi.at[pl.ds(k, kc), :, pl.ds(b * lane, lane)], rb.at[c]).start()

    def zfilt(c, k, kc, s):
        wait(bi.at[pl.ds(k, kc)], rb.at[c])
        x = bi[pl.ds(k, kc)].reshape(kc * zb, 2 * n)
        f = _dot(x, tz[...])
        gg = g[pl.ds(k, kc)].reshape(kc * zb, n)
        v = f * jnp.concatenate([gg, gg], axis=1) * (1.0 / n)
        o = _dot(v, tz[...], ((1,), (1,)))
        bo[pl.ds(k, kc)] = o.reshape(kc, zb, 2 * n)
        for d in range(1, nb):
            t = lax.rem(b + d, nb)
            remote(bo.at[pl.ds(k, kc), :, pl.ds(t * lane, lane)], vi.at[pl.ds(k, kc), pl.ds(b * zb, zb)],
                   s, rbo.at[c if kc > 1 else nk - 1 + NP], (t, a)).start()
        local(bo.at[pl.ds(k, kc), :, pl.ds(b * lane, lane)], vi.at[pl.ds(k, kc), pl.ds(b * zb, zb)], rbo.at[c if kc > 1 else nk - 1 + NP]).start()

    def yinv(c, k, kc, s, pieces=1):
        wait(vi.at[pl.ds(k, kc)], rbo.at[c])
        ydft(vi, iy, k, kc, 1.0 / n, -1.0)
        yc = ya // pieces
        for p in range(pieces):
            dst = aox.at[pl.ds(0, 1)] if kc == 1 else ao.at[pl.ds(k, kc), a, pl.ds(p * yc, yc)]
            for d in range(1, na):
                t = lax.rem(a + d, na)
                remote(iy.at[pl.ds(k, kc), pl.ds(t * ya + p * yc, yc)], dst, s, rao.at[c + p], (b, t)).start()
            local(iy.at[pl.ds(k, kc), pl.ds(a * ya + p * yc, yc)], dst, rao.at[c + p]).start()

    ao2 = ao.reshape(slots * na * ya, lane)
    aox2 = aox.reshape(8 * ya, lane)
    m = GC * KC * na
    ly = 8

    def xinv(p, last):
        extra = p == PX
        trow = 2 * m * p + (16 if p > PX else 0)
        table = txi[trow:trow + 2 * m + (16 if extra else 0), :]
        srcs = [(ao2, p * m * ya, m)] + ([(aox2, 0, 8)] if extra else [])

        def body(j, _):
            if last:
                pc = j * ly // (ya // NP)

                if j * ly % (ya // NP) == 0:
                    wait(ao.at[pl.ds(0, KC), :, pl.ds(0, ya // NP)], rao.at[nk - 1 + pc])
            cols = []
            for h in range(ly // 2):
                parts = []
                for src, first, r in srcs:
                    lo = lanes((r, lane))
                    y = first + ly * j + 2 * h
                    f = src[pl.ds(y, r, stride=ya), :]
                    q = src[pl.ds(y + 1, r, stride=ya), :]
                    parts += [jnp.where(lo, f, pltpu.roll(q, zb, 1)), jnp.where(lo, pltpu.roll(f, zb, 1), q)]
                cols.append(jnp.concatenate(parts, axis=0))
            part = _dot(jnp.concatenate(cols, axis=1), table, ((0,), (0,)))
            if last:
                out[j][...] = w[j * ly * zb:(j + 1) * ly * zb, :] + part
                return 0
            w[pl.ds(pl.multiple_of(j * (ly * zb), ly * zb), ly * zb), :] += part
            return 0

        for c in range(GC * p, GC * (p + 1) - (1 if last else 0)):
            wait(ao.at[pl.ds(0, KC)], rao.at[c])
        if extra:
            wait(aox.at[0], rao.at[nk - 1 + NP])
        if last:
            for j in range(ya // ly):
                body(j, 0)
        else:
            lax.fori_loop(0, ya // ly, body, 0)

    def send_extra():
        xsx, aix = xs.at[pl.ds(xrow, 1)], ai.at[pl.ds(slots, 1), pl.ds(a * ya, ya)]
        to_ex = remote(xsx, aix, ssem.at[4], ra.at[nk], (b, ex))
        to_me = local(xsx, aix, ra.at[nk])
        send_g = remote(g_hbm.at[slots], g.at[own + a], ssem.at[8], rg, (b, na - 1))

        @pl.when(a != ex)
        def _():
            to_ex.start()

        @pl.when(a == ex)
        def _():
            to_me.start()

        @pl.when(a < ex)
        def _():
            send_g.start()

    def step(t, _):
        @pl.when(t < nk)
        def _():
            yfwd(t, t * KC, KC, ssem.at[1])

        @pl.when(t < nk - 2)
        def _():
            send_a(t + 2, (t + 2) * KC, KC, 0, ya)

        @pl.when(t == 1)
        def _():
            send_extra()

        @pl.when((t == TX) & (a == ex))
        def _():
            yfwd(nk, slots, 1, ssem.at[5])

        @pl.when(t == LZ)
        def _():
            for i in (3, 4, 5):
                loads[i].wait()

            @pl.when(a < na - 1)
            def _():
                load_g.wait()

        @pl.when((t == LZ + own // KC) & (a == na - 1))
        def _():
            wait(g.at[pl.ds(own, ex)], rg)

        @pl.when((t >= LZ) & (t < nk + LZ))
        def _():
            zfilt(t - LZ, (t - LZ) * KC, KC, ssem.at[2])

        @pl.when((t == TX + LZ) & (a == ex))
        def _():
            zfilt(nk, slots, 1, ssem.at[6])

        @pl.when(t >= LY)
        def _():
            yinv(t - LY, (t - LY) * KC, KC, ssem.at[3])

        @pl.when((t == TX + LY) & (a == ex))
        def _():
            yinv(nk - 1 + NP, slots, 1, ssem.at[7])

        for p in range(nk // GC - 1):
            @pl.when(t == GC * (p + 1) + LY)
            def _():
                if p == 0:
                    loads[1].wait()
                xinv(p, False)
        return 0

    lax.fori_loop(0, nk + LY - 1, step, 0)
    yinv(nk - 1, (nk - 1) * KC, KC, ssem.at[3], NP)
    xinv(nk // GC - 1, True)

    sa = xs.at[pl.ds(0, (na - 1) * slots)]
    sb = yf.at[pl.ds(0, slots), pl.ds(0, (nb - 1) * zb)]
    wait(sa, ssem.at[0])
    wait(sb, ssem.at[1])
    wait(sb, ssem.at[2])
    wait(sa, ssem.at[3])

    @pl.when(a != ex)
    def _():
        wait(xs.at[0], ssem.at[4])

    @pl.when(a == ex)
    def _():
        wait(yf.at[0, pl.ds(0, (nb - 1) * zb)], ssem.at[5])
        wait(yf.at[0, pl.ds(0, (nb - 1) * zb)], ssem.at[6])
        wait(xs.at[pl.ds(0, na - 1)], ssem.at[7])

    @pl.when(a < ex)
    def _():
        wait(g.at[0], ssem.at[8])


def solution(mesh):
    na, nb = mesh.shape["a"], mesh.shape["b"]

    def body(u, g):
        n, ya, zb = u.shape
        kl = g.shape[0]
        own = _plan(n, na, kl)[2]
        tabs = _tables(n, na, nb, kl)
        ut = jnp.transpose(u, (1, 2, 0)).reshape(ya * zb, n)
        nk = (kl - 1) // KC
        vm = lambda *s: pltpu.VMEM(s, F32)
        dma = lambda *s: pltpu.SemaphoreType.DMA(s)
        hbm = pl.BlockSpec(memory_space=pl.ANY)
        w = pl.pallas_call(
            functools.partial(_kernel, n, na, nb, kl, own),
            name="fftfilter",
            out_shape=[jax.ShapeDtypeStruct((8 * zb, n), F32)] * (ya // 8),
            in_specs=[hbm] * 3,
            out_specs=[pl.BlockSpec(memory_space=pltpu.VMEM)] * (ya // 8),
            scratch_shapes=[
                vm(ya * zb, n), vm(kl, zb, n), *[vm(*t.shape) for t in tabs[:3]], vm(2 * n, 2 * n),
                vm(tabs[0].shape[0] // 2, ya, 2 * zb), vm(kl, n, 2 * zb), vm(kl, n, 2 * zb),
                vm(kl, zb, 2 * n), vm(kl, zb, 2 * n), vm(kl, n, 2 * zb), vm(kl, n, 2 * zb),
                vm(kl - 1, na, ya, 2 * zb), vm(8, ya, 2 * zb), vm(ya * zb, n),
                dma(7), dma(ya // 4), dma(9),
                dma(nk + 1), dma(nk + 1), dma(nk + NP), dma(nk + NP), pltpu.SemaphoreType.DMA,
            ],
            compiler_params=pltpu.CompilerParams(
                collective_id=0, has_side_effects=True, vmem_limit_bytes=54000000),
        )(ut, g, jnp.asarray(np.concatenate(tabs)))
        return jnp.transpose(jnp.concatenate(w).reshape(ya, zb, n), (2, 0, 1))

    return jax.shard_map(body, mesh=mesh, in_specs=(P(None, "a", "b"), P("a", "b", None)),
                         out_specs=P(None, "a", "b"), check_vma=False)
```

```python
import functools
import math
import numpy as np
import jax
import jax.numpy as jnp
from jax import lax
from jax.experimental import pallas as pl
from jax.experimental.pallas import tpu as pltpu
from jax.sharding import PartitionSpec as P

HI = lax.Precision.HIGHEST
MESH = pl.DeviceIdType.MESH
F32 = jnp.float32
KC = 2
LZ = 2
LY = 4
TX = 5
PASSES = (8, 12)


def _trig(n, rows, cols):
    r = np.arange(rows)[:, None]
    c = np.arange(cols)[None, :]
    ang = ((r * c) % n).astype(np.float32) * np.float32(2.0 * math.pi / n)
    ang = ang.astype(np.float64)
    return np.cos(ang).astype(np.float32), np.sin(ang).astype(np.float32)


def _plan(n, na, kl):
    modes = n // 2 + 1
    slots = kl - 1
    own = modes - kl * (na - 1)
    assert own + na - 2 == slots and slots % KC == 0
    kx = kl * np.arange(na)[:, None] + np.arange(slots)[None, :]
    kx[na - 1, own:] = kl * np.arange(na - 2) + slots
    return kx, kl * (na - 2) + slots, own


def _tables(n, na, nb, kl):
    kx, extra, _ = _plan(n, na, kl)
    c, s = _trig(n, n, n)

    def rows(t):
        last = np.zeros((na, n), np.float32)
        last[na - 2] = t[extra]
        return np.concatenate([t[kx.T.reshape(-1)], last])

    m = KC * na
    fc, fs = rows(c), rows(-s)
    tx = np.concatenate([fc[:m], fs[:m], fc[m:], fs[m:]])
    wgt = np.where((np.arange(n) == 0) | (np.arange(n) == n // 2), 1.0, 2.0).astype(np.float32)[:, None] / np.float32(n)
    wc, ws = c * wgt, -s * wgt
    wc, ws = rows(wc), rows(ws)
    txi = []
    for lo, hi in zip((0,) + PASSES, PASSES + (kl,)):
        txi += [wc[lo * na:hi * na], ws[lo * na:hi * na]]
    ty = np.concatenate([c, s], axis=0)
    zb = n // nb
    tz = []
    for b in range(nb):
        cb, sb = c[b * zb:(b + 1) * zb], s[b * zb:(b + 1) * zb]
        tz += [np.concatenate([cb, -sb], axis=1), np.concatenate([sb, cb], axis=1)]
    tz = np.concatenate(tz, axis=0)
    return [np.ascontiguousarray(t, dtype=np.float32) for t in (tx, np.concatenate(txi), ty, tz[:, :n], tz[:, n:])]


def _dot(p, q, dims=((1,), (0,))):
    return lax.dot_general(p, q, (dims, ((), ())), precision=HI, preferred_element_type=F32)


def _kernel(n, na, nb, kl, own, u_hbm, g_hbm, tab_hbm, *refs):
    out, refs = refs[:n // na // 8], refs[n // na // 8:]
    (u, g, tx, txi, ty, tz, xs, ai, yf, bi, bo, vi, iy, ao, w,
            lsem, usem, ssem, ra, rb, rbo, rao, rg) = refs
    a, b = lax.axis_index("a"), lax.axis_index("b")
    ya, zb = n // na, n // nb
    slots = kl - 1
    n2 = slots // KC - 1
    nk = n2 + KC
    ex = na - 2
    rows = 4 * zb
    nj = ya * zb // rows
    lane = 2 * zb

    def local(src, dst, sem):
        return pltpu.make_async_copy(src, dst, sem)

    def remote(src, dst, s, r, t):
        return pltpu.make_async_remote_copy(src, dst, s, r, device_id=t, device_id_type=MESH)

    def wait(ref, sem):
        local(ref, ref, sem).wait()

    bar = pltpu.get_barrier_semaphore()
    for d in range(1, na):
        pl.semaphore_signal(bar, inc=1, device_id=(b, lax.rem(a + d, na)), device_id_type=MESH)
    for d in range(1, nb):
        pl.semaphore_signal(bar, inc=1, device_id=(lax.rem(b + d, nb), a), device_id_type=MESH)

    def load_u(j):
        at = pl.ds(pl.multiple_of(j * rows, rows), rows)
        return local(u_hbm.at[at], u.at[at], usem.at[j])

    loads, at = [], 0
    for d in (tx, txi, ty, tz.at[:, pl.ds(0, n)], tz.at[:, pl.ds(n, n)]):
        loads.append(local(tab_hbm.at[pl.ds(at, d.shape[0])], d, lsem.at[len(loads)]))
        at += d.shape[0]
    loads.append(local(g_hbm.at[pl.ds(0, own)], g.at[pl.ds(0, own)], lsem.at[5]))
    load_g = local(g_hbm.at[pl.ds(own, kl - own)], g.at[pl.ds(own, kl - own)], lsem.at[6])
    loads[0].start()
    for j in range(nj):
        load_u(j).start()
    for cp in loads[1:]:
        cp.start()

    @pl.when(a < na - 1)
    def _():
        load_g.start()

    def lanes(shape):
        return lax.broadcasted_iota(jnp.int32, shape, 1) < zb

    xs2 = xs.reshape(kl * na * ya, lane)

    def send_a(c, k, kc):
        for d in range(1, na):
            t = lax.rem(a + d, na)
            remote(xs.at[pl.ds(k, kc), t], ai.at[pl.ds(k, kc), pl.ds(a * ya, ya)], ssem.at[0], ra.at[c], (b, t)).start()
        local(xs.at[pl.ds(k, kc), a], ai.at[pl.ds(k, kc), pl.ds(a * ya, ya)], ra.at[c]).start()

    def xfwd(r0, nr, first):
        lo = lanes((nr, lane))

        def body(j, _):
            if first:
                load_u(j).wait()
            r = _dot(tx[2 * r0:2 * (r0 + nr), :], u[pl.ds(pl.multiple_of(j * rows, rows), rows), :], ((1,), (1,)))
            for h in range(2):
                re = r[:nr, lane * h:lane * (h + 1)]
                im = r[nr:, lane * h:lane * (h + 1)]
                y = r0 * ya + 4 * j + 2 * h
                xs2[pl.ds(y, nr, stride=ya), :] = jnp.where(lo, re, pltpu.roll(im, zb, 1))
                xs2[pl.ds(y + 1, nr, stride=ya), :] = jnp.where(lo, pltpu.roll(re, zb, 1), im)
            return 0

        lax.fori_loop(0, nj, body, 0)

    loads[0].wait()
    xfwd(0, KC * na, True)
    pl.semaphore_wait(bar, na + nb - 2)
    send_a(0, 0, KC)
    xfwd(KC * na, (kl - KC) * na, False)
    send_a(1, KC, KC)
    ao[slots, 0:ex] = jnp.zeros((ex, ya, lane), F32)
    ao[slots, ex + 1:na] = jnp.zeros((na - ex - 1, ya, lane), F32)
    w[...] = jnp.zeros_like(w)
    loads[2].wait()

    def ydft(src, dst, k, kc, scale, sign):
        x = jnp.concatenate([src[k + i] for i in range(kc)], axis=1)
        if scale is not None:
            x = x * scale
        r = _dot(ty[...], x)
        lo = lanes((n, lane))
        for i in range(kc):
            p = r[:n, lane * i:lane * (i + 1)]
            q = pltpu.roll(r[n:, lane * i:lane * (i + 1)], zb, 1)
            dst[k + i] = p + jnp.where(lo, sign * q, -sign * q)

    def yfwd(c, k, kc, s):
        wait(ai.at[pl.ds(k, kc)], ra.at[c])
        ydft(ai, yf, k, kc, None, 1.0)
        for d in range(1, nb):
            t = lax.rem(b + d, nb)
            remote(yf.at[pl.ds(k, kc), pl.ds(t * zb, zb)], bi.at[pl.ds(k, kc), :, pl.ds(b * lane, lane)],
                   s, rb.at[c], (t, a)).start()
        local(yf.at[pl.ds(k, kc), pl.ds(b * zb, zb)], bi.at[pl.ds(k, kc), :, pl.ds(b * lane, lane)], rb.at[c]).start()

    def zfilt(c, k, kc, s):
        wait(bi.at[pl.ds(k, kc)], rb.at[c])
        x = bi[pl.ds(k, kc)].reshape(kc * zb, 2 * n)
        f = _dot(x, tz[...])
        gg = g[pl.ds(k, kc)].reshape(kc * zb, n)
        v = f * jnp.concatenate([gg, gg], axis=1) * (1.0 / n)
        o = _dot(v, tz[...], ((1,), (1,)))
        bo[pl.ds(k, kc)] = o.reshape(kc, zb, 2 * n)
        for d in range(1, nb):
            t = lax.rem(b + d, nb)
            remote(bo.at[pl.ds(k, kc), :, pl.ds(t * lane, lane)], vi.at[pl.ds(k, kc), pl.ds(b * zb, zb)],
                   s, rbo.at[c], (t, a)).start()
        local(bo.at[pl.ds(k, kc), :, pl.ds(b * lane, lane)], vi.at[pl.ds(k, kc), pl.ds(b * zb, zb)], rbo.at[c]).start()

    def yinv(c, k, kc, s):
        wait(vi.at[pl.ds(k, kc)], rbo.at[c])
        ydft(vi, iy, k, kc, 1.0 / n, -1.0)
        for d in range(1, na):
            t = lax.rem(a + d, na)
            remote(iy.at[pl.ds(k, kc), pl.ds(t * ya, ya)], ao.at[pl.ds(k, kc), a], s, rao.at[c], (b, t)).start()
        local(iy.at[pl.ds(k, kc), pl.ds(a * ya, ya)], ao.at[pl.ds(k, kc), a], rao.at[c]).start()

    ao2 = ao.reshape(kl * na * ya, lane)
    ly = 8

    def xinv(k0, k1, last):
        m = (k1 - k0) * na
        lo = lanes((m, lane))
        table = txi[2 * k0 * na:2 * k1 * na, :]

        def body(j, _):
            cols = []
            for h in range(ly // 2):
                y = k0 * na * ya + ly * j + 2 * h
                p = ao2[pl.ds(y, m, stride=ya), :]
                q = ao2[pl.ds(y + 1, m, stride=ya), :]
                cols.append(jnp.concatenate(
                    [jnp.where(lo, p, pltpu.roll(q, zb, 1)), jnp.where(lo, pltpu.roll(p, zb, 1), q)], axis=0))
            part = _dot(jnp.concatenate(cols, axis=1), table, ((0,), (0,)))
            if last:
                out[j][...] = w[j * ly * zb:(j + 1) * ly * zb, :] + part
                return 0
            w[pl.ds(pl.multiple_of(j * (ly * zb), ly * zb), ly * zb), :] += part
            return 0

        for k in range(k0, k1):
            if k < KC * n2:
                if k % KC == 0:
                    wait(ao.at[pl.ds(0, KC)], rao.at[k // KC])
            elif k < slots:
                wait(ao.at[0], rao.at[k - n2])
            else:
                wait(ao.at[0, 0], rao.at[k - n2])
        if last:
            for j in range(ya // ly):
                body(j, 0)
        else:
            lax.fori_loop(0, ya // ly, body, 0)

    def send_extra():
        xsx, aix = xs.at[pl.ds(slots, 1), ex], ai.at[pl.ds(slots, 1), pl.ds(a * ya, ya)]
        to_ex = remote(xsx, aix, ssem.at[4], ra.at[nk], (b, ex))
        to_me = local(xsx, aix, ra.at[nk])
        send_g = remote(g_hbm.at[slots], g.at[own + a], ssem.at[8], rg, (b, na - 1))

        @pl.when(a != ex)
        def _():
            to_ex.start()

        @pl.when(a == ex)
        def _():
            to_me.start()

        @pl.when(a < ex)
        def _():
            send_g.start()

    def stage(f, t, sem, sem_extra):
        @pl.when((t >= 0) & (t < n2))
        def _():
            f(t, t * KC, KC, ssem.at[sem])

        extra = (t == TX) & (a == ex)

        @pl.when(((t >= n2) & (t < nk)) | extra)
        def _():
            k = jnp.where(t == TX, slots, t + n2 * (KC - 1))
            f(k - n2 * (KC - 1), k, 1, ssem.at[jnp.where(t == TX, sem_extra, sem)])

    def step(t, _):
        stage(yfwd, t, 1, 5)

        @pl.when(t + 2 < n2)
        def _():
            send_a(t + 2, (t + 2) * KC, KC)

        @pl.when((t + 2 >= n2) & (t + 2 < nk))
        def _():
            send_a(t + 2, t + 2 + n2 * (KC - 1), 1)

        @pl.when(t == 1)
        def _():
            send_extra()

        @pl.when(t == LZ)
        def _():
            for i in (3, 4, 5):
                loads[i].wait()

            @pl.when(a < na - 1)
            def _():
                load_g.wait()

        @pl.when((t == LZ + own // KC) & (a == na - 1))
        def _():
            wait(g.at[pl.ds(own, ex)], rg)

        stage(zfilt, t - LZ, 2, 6)
        stage(yinv, t - LY, 3, 7)

        @pl.when(t == PASSES[0] // KC + LY)
        def _():
            loads[1].wait()
            xinv(0, PASSES[0], False)
        return 0

    lax.fori_loop(0, nk + LY, step, 0)
    for k0, k1 in zip(PASSES, PASSES[1:] + (kl,)):
        xinv(k0, k1, k1 == kl)

    sa = xs.at[pl.ds(0, slots), pl.ds(0, na - 1)]
    sb = yf.at[pl.ds(0, slots), pl.ds(0, (nb - 1) * zb)]
    wait(sa, ssem.at[0])
    wait(sb, ssem.at[1])
    wait(sb, ssem.at[2])
    wait(sa, ssem.at[3])

    @pl.when(a != ex)
    def _():
        wait(xs.at[0, 0], ssem.at[4])

    @pl.when(a == ex)
    def _():
        wait(yf.at[0, pl.ds(0, (nb - 1) * zb)], ssem.at[5])
        wait(yf.at[0, pl.ds(0, (nb - 1) * zb)], ssem.at[6])
        wait(xs.at[0, pl.ds(0, na - 1)], ssem.at[7])

    @pl.when(a < ex)
    def _():
        wait(g.at[0], ssem.at[8])


def solution(mesh):
    na, nb = mesh.shape["a"], mesh.shape["b"]

    def body(u, g):
        n, ya, zb = u.shape
        kl = g.shape[0]
        own = _plan(n, na, kl)[2]
        tabs = _tables(n, na, nb, kl)
        ut = jnp.transpose(u, (1, 2, 0)).reshape(ya * zb, n)
        nk = (kl - 1) // KC + KC
        vm = lambda *s: pltpu.VMEM(s, F32)
        dma = lambda *s: pltpu.SemaphoreType.DMA(s)
        hbm = pl.BlockSpec(memory_space=pl.ANY)
        w = pl.pallas_call(
            functools.partial(_kernel, n, na, nb, kl, own),
            name="fftfilter",
            out_shape=[jax.ShapeDtypeStruct((8 * zb, n), F32)] * (ya // 8),
            in_specs=[hbm] * 3,
            out_specs=[pl.BlockSpec(memory_space=pltpu.VMEM)] * (ya // 8),
            scratch_shapes=[
                vm(ya * zb, n), vm(kl, zb, n), *[vm(*t.shape) for t in tabs[:3]], vm(2 * n, 2 * n),
                vm(kl, na, ya, 2 * zb), vm(kl, n, 2 * zb), vm(kl, n, 2 * zb),
                vm(kl, zb, 2 * n), vm(kl, zb, 2 * n), vm(kl, n, 2 * zb), vm(kl, n, 2 * zb),
                vm(kl, na, ya, 2 * zb), vm(ya * zb, n),
                dma(7), dma(ya // 4), dma(9),
                dma(nk), dma(nk), dma(nk), dma(nk), pltpu.SemaphoreType.DMA,
            ],
            compiler_params=pltpu.CompilerParams(
                collective_id=0, has_side_effects=True, vmem_limit_bytes=54000000),
        )(ut, g, jnp.asarray(np.concatenate(tabs)))
        return jnp.transpose(jnp.concatenate(w).reshape(ya, zb, n), (2, 0, 1))

    return jax.shard_map(body, mesh=mesh, in_specs=(P(None, "a", "b"), P("a", "b", None)),
                         out_specs=P(None, "a", "b"), check_vma=False)
```

```python
import functools
import math
import numpy as np
import jax
import jax.numpy as jnp
from jax import lax
from jax.experimental import pallas as pl
from jax.experimental.pallas import tpu as pltpu
from jax.sharding import PartitionSpec as P

HI = lax.Precision.HIGHEST
MESH = pl.DeviceIdType.MESH
F32 = jnp.float32
KC = 2
LZ = 2
LY = 4
TX = 5
XCUT = 8
PASSES = (8, 12)


def _trig(n, rows, cols):
    r = np.arange(rows)[:, None]
    c = np.arange(cols)[None, :]
    ang = ((r * c) % n).astype(np.float32) * np.float32(2.0 * math.pi / n)
    ang = ang.astype(np.float64)
    return np.cos(ang).astype(np.float32), np.sin(ang).astype(np.float32)


def _plan(n, na, kl):
    modes = n // 2 + 1
    slots = kl - 1
    own = modes - kl * (na - 1)
    assert own + na - 2 == slots and slots % KC == 0
    kx = kl * np.arange(na)[:, None] + np.arange(slots)[None, :]
    kx[na - 1, own:] = kl * np.arange(na - 2) + slots
    return kx, kl * (na - 2) + slots, own


def _tables(n, na, nb, kl):
    kx, extra, _ = _plan(n, na, kl)
    c, s = _trig(n, n, n)

    def rows(t):
        last = np.zeros((na, n), np.float32)
        last[na - 2] = t[extra]
        return np.concatenate([t[kx.T.reshape(-1)], last])

    m = KC * na
    fc, fs = rows(c), rows(-s)
    cut = XCUT * na
    tx = np.concatenate([fc[:m], fs[:m], fc[m:cut], fs[m:cut], fc[cut:], fs[cut:]])
    wgt = np.where((np.arange(n) == 0) | (np.arange(n) == n // 2), 1.0, 2.0).astype(np.float32)[:, None] / np.float32(n)
    wc, ws = c * wgt, -s * wgt
    wc, ws = rows(wc), rows(ws)
    txi = []
    for lo, hi in zip((0,) + PASSES, PASSES + (kl,)):
        txi += [wc[lo * na:hi * na], ws[lo * na:hi * na]]
    ty = np.concatenate([c, s], axis=0)
    zb = n // nb
    tz = []
    for b in range(nb):
        cb, sb = c[b * zb:(b + 1) * zb], s[b * zb:(b + 1) * zb]
        tz += [np.concatenate([cb, -sb], axis=1), np.concatenate([sb, cb], axis=1)]
    tz = np.concatenate(tz, axis=0)
    return [np.ascontiguousarray(t, dtype=np.float32) for t in (tx, np.concatenate(txi), ty, tz[:, :n], tz[:, n:])]


def _dot(p, q, dims=((1,), (0,))):
    return lax.dot_general(p, q, (dims, ((), ())), precision=HI, preferred_element_type=F32)


def _kernel(n, na, nb, kl, own, u_hbm, g_hbm, tab_hbm, *refs):
    out, refs = refs[:n // na // 8], refs[n // na // 8:]
    (u, g, tx, txi, ty, tz, xs, ai, yf, bi, bo, vi, iy, ao, w,
            lsem, usem, ssem, ra, rb, rbo, rao, rg) = refs
    a, b = lax.axis_index("a"), lax.axis_index("b")
    ya, zb = n // na, n // nb
    slots = kl - 1
    n2 = slots // KC - 1
    nk = n2 + KC
    ex = na - 2
    rows = 4 * zb
    nj = ya * zb // rows
    lane = 2 * zb

    def local(src, dst, sem):
        return pltpu.make_async_copy(src, dst, sem)

    def remote(src, dst, s, r, t):
        return pltpu.make_async_remote_copy(src, dst, s, r, device_id=t, device_id_type=MESH)

    def wait(ref, sem):
        local(ref, ref, sem).wait()

    bar = pltpu.get_barrier_semaphore()
    for d in range(1, na):
        pl.semaphore_signal(bar, inc=1, device_id=(b, lax.rem(a + d, na)), device_id_type=MESH)
    for d in range(1, nb):
        pl.semaphore_signal(bar, inc=1, device_id=(lax.rem(b + d, nb), a), device_id_type=MESH)

    def load_u(j):
        at = pl.ds(pl.multiple_of(j * rows, rows), rows)
        return local(u_hbm.at[at], u.at[at], usem.at[j])

    loads, at = [], 0
    for d in (tx, txi, ty, tz.at[:, pl.ds(0, n)], tz.at[:, pl.ds(n, n)]):
        loads.append(local(tab_hbm.at[pl.ds(at, d.shape[0])], d, lsem.at[len(loads)]))
        at += d.shape[0]
    loads.append(local(g_hbm.at[pl.ds(0, own)], g.at[pl.ds(0, own)], lsem.at[5]))
    load_g = local(g_hbm.at[pl.ds(own, kl - own)], g.at[pl.ds(own, kl - own)], lsem.at[6])
    loads[0].start()
    for j in range(nj):
        load_u(j).start()
    for cp in loads[1:]:
        cp.start()

    @pl.when(a < na - 1)
    def _():
        load_g.start()

    def lanes(shape):
        return lax.broadcasted_iota(jnp.int32, shape, 1) < zb

    xs2 = xs.reshape(kl * na * ya, lane)

    def send_a(c, k, kc):
        for d in range(1, na):
            t = lax.rem(a + d, na)
            remote(xs.at[pl.ds(k, kc), t], ai.at[pl.ds(k, kc), pl.ds(a * ya, ya)], ssem.at[0], ra.at[c], (b, t)).start()
        local(xs.at[pl.ds(k, kc), a], ai.at[pl.ds(k, kc), pl.ds(a * ya, ya)], ra.at[c]).start()

    def xfwd(r0, nr, first):
        lo = lanes((nr, lane))

        def body(j, _):
            if first:
                load_u(j).wait()
            r = _dot(tx[2 * r0:2 * (r0 + nr), :], u[pl.ds(pl.multiple_of(j * rows, rows), rows), :], ((1,), (1,)))
            for h in range(2):
                re = r[:nr, lane * h:lane * (h + 1)]
                im = r[nr:, lane * h:lane * (h + 1)]
                y = r0 * ya + 4 * j + 2 * h
                xs2[pl.ds(y, nr, stride=ya), :] = jnp.where(lo, re, pltpu.roll(im, zb, 1))
                xs2[pl.ds(y + 1, nr, stride=ya), :] = jnp.where(lo, pltpu.roll(re, zb, 1), im)
            return 0

        lax.fori_loop(0, nj, body, 0)

    loads[0].wait()
    xfwd(0, KC * na, True)
    pl.semaphore_wait(bar, na + nb - 2)
    send_a(0, 0, KC)
    xfwd(KC * na, (XCUT - KC) * na, False)
    send_a(1, KC, KC)
    ao[slots, 0:ex] = jnp.zeros((ex, ya, lane), F32)
    ao[slots, ex + 1:na] = jnp.zeros((na - ex - 1, ya, lane), F32)
    loads[2].wait()

    def ydft(src, dst, k, kc, scale, sign):
        x = jnp.concatenate([src[k + i] for i in range(kc)], axis=1)
        if scale is not None:
            x = x * scale
        r = _dot(ty[...], x)
        lo = lanes((n, lane))
        for i in range(kc):
            p = r[:n, lane * i:lane * (i + 1)]
            q = pltpu.roll(r[n:, lane * i:lane * (i + 1)], zb, 1)
            dst[k + i] = p + jnp.where(lo, sign * q, -sign * q)

    def yfwd(c, k, kc, s):
        wait(ai.at[pl.ds(k, kc)], ra.at[c])
        ydft(ai, yf, k, kc, None, 1.0)
        for d in range(1, nb):
            t = lax.rem(b + d, nb)
            remote(yf.at[pl.ds(k, kc), pl.ds(t * zb, zb)], bi.at[pl.ds(k, kc), :, pl.ds(b * lane, lane)],
                   s, rb.at[c], (t, a)).start()
        local(yf.at[pl.ds(k, kc), pl.ds(b * zb, zb)], bi.at[pl.ds(k, kc), :, pl.ds(b * lane, lane)], rb.at[c]).start()

    def zfilt(c, k, kc, s):
        wait(bi.at[pl.ds(k, kc)], rb.at[c])
        x = bi[pl.ds(k, kc)].reshape(kc * zb, 2 * n)
        f = _dot(x, tz[...])
        gg = g[pl.ds(k, kc)].reshape(kc * zb, n)
        v = f * jnp.concatenate([gg, gg], axis=1) * (1.0 / n)
        o = _dot(v, tz[...], ((1,), (1,)))
        bo[pl.ds(k, kc)] = o.reshape(kc, zb, 2 * n)
        for d in range(1, nb):
            t = lax.rem(b + d, nb)
            remote(bo.at[pl.ds(k, kc), :, pl.ds(t * lane, lane)], vi.at[pl.ds(k, kc), pl.ds(b * zb, zb)],
                   s, rbo.at[c], (t, a)).start()
        local(bo.at[pl.ds(k, kc), :, pl.ds(b * lane, lane)], vi.at[pl.ds(k, kc), pl.ds(b * zb, zb)], rbo.at[c]).start()

    def yinv(c, k, kc, s):
        wait(vi.at[pl.ds(k, kc)], rbo.at[c])
        ydft(vi, iy, k, kc, 1.0 / n, -1.0)
        for d in range(1, na):
            t = lax.rem(a + d, na)
            remote(iy.at[pl.ds(k, kc), pl.ds(t * ya, ya)], ao.at[pl.ds(k, kc), a], s, rao.at[c], (b, t)).start()
        local(iy.at[pl.ds(k, kc), pl.ds(a * ya, ya)], ao.at[pl.ds(k, kc), a], rao.at[c]).start()

    ao2 = ao.reshape(kl * na * ya, lane)
    ly = 8

    def xinv(k0, k1, last):
        m = (k1 - k0) * na
        lo = lanes((m, lane))
        table = txi[2 * k0 * na:2 * k1 * na, :]

        def body(j, _):
            cols = []
            for h in range(ly // 2):
                y = k0 * na * ya + ly * j + 2 * h
                p = ao2[pl.ds(y, m, stride=ya), :]
                q = ao2[pl.ds(y + 1, m, stride=ya), :]
                cols.append(jnp.concatenate(
                    [jnp.where(lo, p, pltpu.roll(q, zb, 1)), jnp.where(lo, pltpu.roll(p, zb, 1), q)], axis=0))
            part = _dot(jnp.concatenate(cols, axis=1), table, ((0,), (0,)))
            if last:
                out[j][...] = w[j * ly * zb:(j + 1) * ly * zb, :] + part
                return 0
            w[pl.ds(pl.multiple_of(j * (ly * zb), ly * zb), ly * zb), :] += part
            return 0

        for k in range(k0, k1):
            if k < KC * n2:
                if k % KC == 0:
                    wait(ao.at[pl.ds(0, KC)], rao.at[k // KC])
            elif k < slots:
                wait(ao.at[0], rao.at[k - n2])
            else:
                wait(ao.at[0, 0], rao.at[k - n2])
        if last:
            for j in range(ya // ly):
                body(j, 0)
        else:
            lax.fori_loop(0, ya // ly, body, 0)

    def send_extra():
        xsx, aix = xs.at[pl.ds(slots, 1), ex], ai.at[pl.ds(slots, 1), pl.ds(a * ya, ya)]
        to_ex = remote(xsx, aix, ssem.at[4], ra.at[nk], (b, ex))
        to_me = local(xsx, aix, ra.at[nk])
        send_g = remote(g_hbm.at[slots], g.at[own + a], ssem.at[8], rg, (b, na - 1))

        @pl.when(a != ex)
        def _():
            to_ex.start()

        @pl.when(a == ex)
        def _():
            to_me.start()

        @pl.when(a < ex)
        def _():
            send_g.start()

    def stage(f, t, sem, sem_extra):
        @pl.when((t >= 0) & (t < n2))
        def _():
            f(t, t * KC, KC, ssem.at[sem])

        extra = (t == TX) & (a == ex)

        @pl.when(((t >= n2) & (t < nk)) | extra)
        def _():
            k = jnp.where(t == TX, slots, t + n2 * (KC - 1))
            f(k - n2 * (KC - 1), k, 1, ssem.at[jnp.where(t == TX, sem_extra, sem)])

    def step(t, _):
        stage(yfwd, t, 1, 5)

        @pl.when(t + 2 < n2)
        def _():
            send_a(t + 2, (t + 2) * KC, KC)

        @pl.when((t + 2 >= n2) & (t + 2 < nk))
        def _():
            send_a(t + 2, t + 2 + n2 * (KC - 1), 1)

        @pl.when(t == 1)
        def _():
            send_extra()

        @pl.when(t == LZ)
        def _():
            for i in (3, 4, 5):
                loads[i].wait()

            @pl.when(a < na - 1)
            def _():
                load_g.wait()

        @pl.when((t == LZ + own // KC) & (a == na - 1))
        def _():
            wait(g.at[pl.ds(own, ex)], rg)

        stage(zfilt, t - LZ, 2, 6)
        stage(yinv, t - LY, 3, 7)

        @pl.when(t == PASSES[0] // KC + LY)
        def _():
            loads[1].wait()
            xinv(0, PASSES[0], False)
        return 0

    yfwd(0, 0, KC, ssem.at[1])
    xfwd(XCUT * na, (kl - XCUT) * na, False)
    send_a(2, 2 * KC, KC)
    w[...] = jnp.zeros_like(w)
    lax.fori_loop(1, nk + LY, step, 0)
    for k0, k1 in zip(PASSES, PASSES[1:] + (kl,)):
        xinv(k0, k1, k1 == kl)

    sa = xs.at[pl.ds(0, slots), pl.ds(0, na - 1)]
    sb = yf.at[pl.ds(0, slots), pl.ds(0, (nb - 1) * zb)]
    wait(sa, ssem.at[0])
    wait(sb, ssem.at[1])
    wait(sb, ssem.at[2])
    wait(sa, ssem.at[3])

    @pl.when(a != ex)
    def _():
        wait(xs.at[0, 0], ssem.at[4])

    @pl.when(a == ex)
    def _():
        wait(yf.at[0, pl.ds(0, (nb - 1) * zb)], ssem.at[5])
        wait(yf.at[0, pl.ds(0, (nb - 1) * zb)], ssem.at[6])
        wait(xs.at[0, pl.ds(0, na - 1)], ssem.at[7])

    @pl.when(a < ex)
    def _():
        wait(g.at[0], ssem.at[8])


def solution(mesh):
    na, nb = mesh.shape["a"], mesh.shape["b"]

    def body(u, g):
        n, ya, zb = u.shape
        kl = g.shape[0]
        own = _plan(n, na, kl)[2]
        tabs = _tables(n, na, nb, kl)
        ut = jnp.transpose(u, (1, 2, 0)).reshape(ya * zb, n)
        nk = (kl - 1) // KC + KC
        vm = lambda *s: pltpu.VMEM(s, F32)
        dma = lambda *s: pltpu.SemaphoreType.DMA(s)
        hbm = pl.BlockSpec(memory_space=pl.ANY)
        w = pl.pallas_call(
            functools.partial(_kernel, n, na, nb, kl, own),
            name="fftfilter",
            out_shape=[jax.ShapeDtypeStruct((8 * zb, n), F32)] * (ya // 8),
            in_specs=[hbm] * 3,
            out_specs=[pl.BlockSpec(memory_space=pltpu.VMEM)] * (ya // 8),
            scratch_shapes=[
                vm(ya * zb, n), vm(kl, zb, n), *[vm(*t.shape) for t in tabs[:3]], vm(2 * n, 2 * n),
                vm(kl, na, ya, 2 * zb), vm(kl, n, 2 * zb), vm(kl, n, 2 * zb),
                vm(kl, zb, 2 * n), vm(kl, zb, 2 * n), vm(kl, n, 2 * zb), vm(kl, n, 2 * zb),
                vm(kl, na, ya, 2 * zb), vm(ya * zb, n),
                dma(7), dma(ya // 4), dma(9),
                dma(nk), dma(nk), dma(nk), dma(nk), pltpu.SemaphoreType.DMA,
            ],
            compiler_params=pltpu.CompilerParams(
                collective_id=0, has_side_effects=True, vmem_limit_bytes=54000000),
        )(ut, g, jnp.asarray(np.concatenate(tabs)))
        return jnp.transpose(jnp.concatenate(w).reshape(ya, zb, n), (2, 0, 1))

    return jax.shard_map(body, mesh=mesh, in_specs=(P(None, "a", "b"), P("a", "b", None)),
                         out_specs=P(None, "a", "b"), check_vma=False)
```

```python
import functools
import math
import numpy as np
import jax
import jax.numpy as jnp
from jax import lax
from jax.experimental import pallas as pl
from jax.experimental.pallas import tpu as pltpu
from jax.sharding import PartitionSpec as P

HI = lax.Precision.HIGHEST
MESH = pl.DeviceIdType.MESH
F32 = jnp.float32
KC = 2
LZ = 2
LY = 4
TX = 5
XCUT = 8
PASSES = (8, 12)


def _trig(n, rows, cols):
    r = np.arange(rows)[:, None]
    c = np.arange(cols)[None, :]
    ang = ((r * c) % n).astype(np.float32) * np.float32(2.0 * math.pi / n)
    ang = ang.astype(np.float64)
    return np.cos(ang).astype(np.float32), np.sin(ang).astype(np.float32)


def _plan(n, na, kl):
    modes = n // 2 + 1
    slots = kl - 1
    own = modes - kl * (na - 1)
    assert own + na - 2 == slots and slots % KC == 0
    kx = kl * np.arange(na)[:, None] + np.arange(slots)[None, :]
    kx[na - 1, own:] = kl * np.arange(na - 2) + slots
    return kx, kl * (na - 2) + slots, own


def _tables(n, na, nb, kl):
    kx, extra, _ = _plan(n, na, kl)
    c, s = _trig(n, n, n)

    def rows(t):
        last = np.zeros((na, n), np.float32)
        last[na - 2] = t[extra]
        return np.concatenate([t[kx.T.reshape(-1)], last])

    m = KC * na
    fc, fs = rows(c), rows(-s)
    cut = XCUT * na
    tx = np.concatenate([fc[:m], fs[:m], fc[m:cut], fs[m:cut], fc[cut:], fs[cut:]])
    wgt = np.where((np.arange(n) == 0) | (np.arange(n) == n // 2), 1.0, 2.0).astype(np.float32)[:, None] / np.float32(n)
    wc, ws = c * wgt, -s * wgt
    wc, ws = rows(wc), rows(ws)
    txi = []
    for lo, hi in zip((0,) + PASSES, PASSES + (kl,)):
        txi += [wc[lo * na:hi * na], ws[lo * na:hi * na]]
    ty = np.concatenate([c, s], axis=0)
    zb = n // nb
    tz = []
    for b in range(nb):
        cb, sb = c[b * zb:(b + 1) * zb], s[b * zb:(b + 1) * zb]
        tz += [np.concatenate([cb, -sb], axis=1), np.concatenate([sb, cb], axis=1)]
    tz = np.concatenate(tz, axis=0)
    return [np.ascontiguousarray(t, dtype=np.float32) for t in (tx, np.concatenate(txi), ty, tz[:, :n], tz[:, n:])]


def _dot(p, q, dims=((1,), (0,))):
    return lax.dot_general(p, q, (dims, ((), ())), precision=HI, preferred_element_type=F32)


def _kernel(n, na, nb, kl, own, u_hbm, g_hbm, tab_hbm, *refs):
    out, refs = refs[:n // na // 8], refs[n // na // 8:]
    (u, g, tx, txi, ty, tz, xs, ai, yf, bi, bo, vi, iy, ao, w,
            lsem, usem, ssem, ra, rb, rbo, rao, rg) = refs
    a, b = lax.axis_index("a"), lax.axis_index("b")
    ya, zb = n // na, n // nb
    slots = kl - 1
    n2 = slots // KC - 1
    nk = n2 + KC
    ex = na - 2
    rows = 4 * zb
    nj = ya * zb // rows
    lane = 2 * zb

    def local(src, dst, sem):
        return pltpu.make_async_copy(src, dst, sem)

    def remote(src, dst, s, r, t):
        return pltpu.make_async_remote_copy(src, dst, s, r, device_id=t, device_id_type=MESH)

    def wait(ref, sem):
        local(ref, ref, sem).wait()

    bar = pltpu.get_barrier_semaphore()
    for d in range(1, na):
        pl.semaphore_signal(bar, inc=1, device_id=(b, lax.rem(a + d, na)), device_id_type=MESH)
    for d in range(1, nb):
        pl.semaphore_signal(bar, inc=1, device_id=(lax.rem(b + d, nb), a), device_id_type=MESH)

    def load_u(j):
        at = pl.ds(pl.multiple_of(j * rows, rows), rows)
        return local(u_hbm.at[at], u.at[at], usem.at[j])

    loads, at = [], 0
    for d in (tx, txi, ty, tz.at[:, pl.ds(0, n)], tz.at[:, pl.ds(n, n)]):
        loads.append(local(tab_hbm.at[pl.ds(at, d.shape[0])], d, lsem.at[len(loads)]))
        at += d.shape[0]
    loads.append(local(g_hbm.at[pl.ds(0, own)], g.at[pl.ds(0, own)], lsem.at[5]))
    load_g = local(g_hbm.at[pl.ds(own, kl - own)], g.at[pl.ds(own, kl - own)], lsem.at[6])
    loads[0].start()
    for j in range(nj):
        load_u(j).start()
    for cp in loads[1:]:
        cp.start()

    @pl.when(a < na - 1)
    def _():
        load_g.start()

    def lanes(shape):
        return lax.broadcasted_iota(jnp.int32, shape, 1) < zb

    xs2 = xs.reshape(kl * na * ya, lane)

    def send_a(c, k, kc):
        for d in range(1, na):
            t = lax.rem(a + d, na)
            remote(xs.at[pl.ds(k, kc), t], ai.at[pl.ds(k, kc), pl.ds(a * ya, ya)], ssem.at[0], ra.at[c], (b, t)).start()
        local(xs.at[pl.ds(k, kc), a], ai.at[pl.ds(k, kc), pl.ds(a * ya, ya)], ra.at[c]).start()

    def xfwd(r0, nr, first):
        lo = lanes((nr, lane))

        def body(j, _):
            if first:
                load_u(j).wait()
            r = _dot(tx[2 * r0:2 * (r0 + nr), :], u[pl.ds(pl.multiple_of(j * rows, rows), rows), :], ((1,), (1,)))
            for h in range(2):
                re = r[:nr, lane * h:lane * (h + 1)]
                im = r[nr:, lane * h:lane * (h + 1)]
                y = r0 * ya + 4 * j + 2 * h
                xs2[pl.ds(y, nr, stride=ya), :] = jnp.where(lo, re, pltpu.roll(im, zb, 1))
                xs2[pl.ds(y + 1, nr, stride=ya), :] = jnp.where(lo, pltpu.roll(re, zb, 1), im)
            return 0

        lax.fori_loop(0, nj, body, 0)

    loads[0].wait()
    xfwd(0, KC * na, True)
    pl.semaphore_wait(bar, na + nb - 2)
    send_a(0, 0, KC)
    xfwd(KC * na, (XCUT - KC) * na, False)
    send_a(1, KC, KC)
    ao[slots, 0:ex] = jnp.zeros((ex, ya, lane), F32)
    ao[slots, ex + 1:na] = jnp.zeros((na - ex - 1, ya, lane), F32)
    loads[2].wait()

    def ydft(src, dst, k, kc, scale, sign):
        x = jnp.concatenate([src[k + i] for i in range(kc)], axis=1)
        if scale is not None:
            x = x * scale
        r = _dot(ty[...], x)
        lo = lanes((n, lane))
        for i in range(kc):
            p = r[:n, lane * i:lane * (i + 1)]
            q = pltpu.roll(r[n:, lane * i:lane * (i + 1)], zb, 1)
            dst[k + i] = p + jnp.where(lo, sign * q, -sign * q)

    def yfwd(c, k, kc, s):
        wait(ai.at[pl.ds(k, kc)], ra.at[c])
        ydft(ai, yf, k, kc, None, 1.0)
        for d in range(1, nb):
            t = lax.rem(b + d, nb)
            remote(yf.at[pl.ds(k, kc), pl.ds(t * zb, zb)], bi.at[pl.ds(k, kc), :, pl.ds(b * lane, lane)],
                   s, rb.at[c], (t, a)).start()
        local(yf.at[pl.ds(k, kc), pl.ds(b * zb, zb)], bi.at[pl.ds(k, kc), :, pl.ds(b * lane, lane)], rb.at[c]).start()

    def zfilt(c, k, kc, s):
        wait(bi.at[pl.ds(k, kc)], rb.at[c])
        x = bi[pl.ds(k, kc)].reshape(kc * zb, 2 * n)
        f = _dot(x, tz[...])
        gg = g[pl.ds(k, kc)].reshape(kc * zb, n)
        v = f * jnp.concatenate([gg, gg], axis=1) * (1.0 / n)
        o = _dot(v, tz[...], ((1,), (1,)))
        bo[pl.ds(k, kc)] = o.reshape(kc, zb, 2 * n)
        for d in range(1, nb):
            t = lax.rem(b + d, nb)
            remote(bo.at[pl.ds(k, kc), :, pl.ds(t * lane, lane)], vi.at[pl.ds(k, kc), pl.ds(b * zb, zb)],
                   s, rbo.at[c], (t, a)).start()
        local(bo.at[pl.ds(k, kc), :, pl.ds(b * lane, lane)], vi.at[pl.ds(k, kc), pl.ds(b * zb, zb)], rbo.at[c]).start()

    def yinv(c, k, kc, s):
        wait(vi.at[pl.ds(k, kc)], rbo.at[c])
        ydft(vi, iy, k, kc, 1.0 / n, -1.0)
        for d in range(1, na):
            t = lax.rem(a + d, na)
            remote(iy.at[pl.ds(k, kc), pl.ds(t * ya, ya)], ao.at[pl.ds(k, kc), a], s, rao.at[c], (b, t)).start()
        local(iy.at[pl.ds(k, kc), pl.ds(a * ya, ya)], ao.at[pl.ds(k, kc), a], rao.at[c]).start()

    ao2 = ao.reshape(kl * na * ya, lane)
    ly = 8

    def xinv(k0, k1, last):
        m = (k1 - k0) * na
        lo = lanes((m, lane))
        table = txi[2 * k0 * na:2 * k1 * na, :]

        def body(j, _):
            cols = []
            for h in range(ly // 2):
                y = k0 * na * ya + ly * j + 2 * h
                p = ao2[pl.ds(y, m, stride=ya), :]
                q = ao2[pl.ds(y + 1, m, stride=ya), :]
                cols.append(jnp.concatenate(
                    [jnp.where(lo, p, pltpu.roll(q, zb, 1)), jnp.where(lo, pltpu.roll(p, zb, 1), q)], axis=0))
            part = _dot(jnp.concatenate(cols, axis=1), table, ((0,), (0,)))
            if last:
                out[j][...] = w[j * ly * zb:(j + 1) * ly * zb, :] + part
                return 0
            w[pl.ds(pl.multiple_of(j * (ly * zb), ly * zb), ly * zb), :] += part
            return 0

        for k in range(k0, k1):
            if k < KC * n2:
                if k % KC == 0:
                    wait(ao.at[pl.ds(0, KC)], rao.at[k // KC])
            elif k < slots:
                wait(ao.at[0], rao.at[k - n2])
            else:
                wait(ao.at[0, 0], rao.at[k - n2])
        if last:
            for j in range(ya // ly):
                body(j, 0)
        else:
            lax.fori_loop(0, ya // ly, body, 0)

    def send_extra():
        xsx, aix = xs.at[pl.ds(slots, 1), ex], ai.at[pl.ds(slots, 1), pl.ds(a * ya, ya)]
        to_ex = remote(xsx, aix, ssem.at[4], ra.at[nk], (b, ex))
        to_me = local(xsx, aix, ra.at[nk])
        send_g = remote(g_hbm.at[slots], g.at[own + a], ssem.at[8], rg, (b, na - 1))

        @pl.when(a != ex)
        def _():
            to_ex.start()

        @pl.when(a == ex)
        def _():
            to_me.start()

        @pl.when(a < ex)
        def _():
            send_g.start()

    def stage(f, t, sem, sem_extra):
        @pl.when((t >= 0) & (t < n2))
        def _():
            f(t, t * KC, KC, ssem.at[sem])

        extra = (t == TX) & (a == ex)

        @pl.when(((t >= n2) & (t < nk)) | extra)
        def _():
            k = jnp.where(t == TX, slots, t + n2 * (KC - 1))
            f(k - n2 * (KC - 1), k, 1, ssem.at[jnp.where(t == TX, sem_extra, sem)])

    def step(t, _):
        stage(yfwd, t, 1, 5)

        @pl.when(t + 3 < n2)
        def _():
            send_a(t + 3, (t + 3) * KC, KC)

        @pl.when((t + 3 >= n2) & (t + 3 < nk))
        def _():
            send_a(t + 3, t + 3 + n2 * (KC - 1), 1)

        @pl.when(t == 1)
        def _():
            send_extra()

        @pl.when(t == LZ)
        def _():
            for i in (3, 4, 5):
                loads[i].wait()

            @pl.when(a < na - 1)
            def _():
                load_g.wait()

        @pl.when((t == LZ + own // KC) & (a == na - 1))
        def _():
            wait(g.at[pl.ds(own, ex)], rg)

        stage(zfilt, t - LZ, 2, 6)
        stage(yinv, t - LY, 3, 7)

        @pl.when(t == PASSES[0] // KC + LY)
        def _():
            loads[1].wait()
            xinv(0, PASSES[0], False)
        return 0

    yfwd(0, 0, KC, ssem.at[1])
    xfwd(XCUT * na, (kl - XCUT) * na, False)
    send_a(2, 2 * KC, KC)
    send_a(3, 3 * KC, KC)
    w[...] = jnp.zeros_like(w)
    lax.fori_loop(1, nk + LY, step, 0)
    for k0, k1 in zip(PASSES, PASSES[1:] + (kl,)):
        xinv(k0, k1, k1 == kl)

    sa = xs.at[pl.ds(0, slots), pl.ds(0, na - 1)]
    sb = yf.at[pl.ds(0, slots), pl.ds(0, (nb - 1) * zb)]
    wait(sa, ssem.at[0])
    wait(sb, ssem.at[1])
    wait(sb, ssem.at[2])
    wait(sa, ssem.at[3])

    @pl.when(a != ex)
    def _():
        wait(xs.at[0, 0], ssem.at[4])

    @pl.when(a == ex)
    def _():
        wait(yf.at[0, pl.ds(0, (nb - 1) * zb)], ssem.at[5])
        wait(yf.at[0, pl.ds(0, (nb - 1) * zb)], ssem.at[6])
        wait(xs.at[0, pl.ds(0, na - 1)], ssem.at[7])

    @pl.when(a < ex)
    def _():
        wait(g.at[0], ssem.at[8])


def solution(mesh):
    na, nb = mesh.shape["a"], mesh.shape["b"]

    def body(u, g):
        n, ya, zb = u.shape
        kl = g.shape[0]
        own = _plan(n, na, kl)[2]
        tabs = _tables(n, na, nb, kl)
        ut = jnp.transpose(u, (1, 2, 0)).reshape(ya * zb, n)
        nk = (kl - 1) // KC + KC
        vm = lambda *s: pltpu.VMEM(s, F32)
        dma = lambda *s: pltpu.SemaphoreType.DMA(s)
        hbm = pl.BlockSpec(memory_space=pl.ANY)
        w = pl.pallas_call(
            functools.partial(_kernel, n, na, nb, kl, own),
            name="fftfilter",
            out_shape=[jax.ShapeDtypeStruct((8 * zb, n), F32)] * (ya // 8),
            in_specs=[hbm] * 3,
            out_specs=[pl.BlockSpec(memory_space=pltpu.VMEM)] * (ya // 8),
            scratch_shapes=[
                vm(ya * zb, n), vm(kl, zb, n), *[vm(*t.shape) for t in tabs[:3]], vm(2 * n, 2 * n),
                vm(kl, na, ya, 2 * zb), vm(kl, n, 2 * zb), vm(kl, n, 2 * zb),
                vm(kl, zb, 2 * n), vm(kl, zb, 2 * n), vm(kl, n, 2 * zb), vm(kl, n, 2 * zb),
                vm(kl, na, ya, 2 * zb), vm(ya * zb, n),
                dma(7), dma(ya // 4), dma(9),
                dma(nk), dma(nk), dma(nk), dma(nk), pltpu.SemaphoreType.DMA,
            ],
            compiler_params=pltpu.CompilerParams(
                collective_id=0, has_side_effects=True, vmem_limit_bytes=54000000),
        )(ut, g, jnp.asarray(np.concatenate(tabs)))
        return jnp.transpose(jnp.concatenate(w).reshape(ya, zb, n), (2, 0, 1))

    return jax.shard_map(body, mesh=mesh, in_specs=(P(None, "a", "b"), P("a", "b", None)),
                         out_specs=P(None, "a", "b"), check_vma=False)
```
